32 devices in a mesh: vert: 8 (over z, y), col: 4 (over x, core).
Axes of the slice: x: 2, y: 2, z: 4, core: 2. Of those that a mesh axis runs over, the one named last changes fastest.
Arguments:
- coeffs: bfloat16 [64, 400], P(('vert', 'col')), may hold values from -6 to 6
- shape_basis: bfloat16 [400, 3, 656], P('col', None, 'vert'), may hold values from -0.3125 to 0.3125
- template: float32 [3, 656], P(None, 'vert'), may hold values from -6 to 6
- regressor: float32 [55, 656], P(None, 'vert'), may hold values from -0.5 to 0.5
- quaternions: float32 [64, 4, 55], P(('vert', 'col')), may hold values from -1.5 to 1.5, as said below
- translation: float32 [64, 3], P(('vert', 'col')), may hold values from -6 to 6
- parents: int32 [55], replicated, may hold values from 0 to 53, as said below
- skin_index: int32 [656, 4], P('vert'), may hold values from 0 to 54, all different within a row
- skin_raw: float32 [656, 4], P('vert'), may hold values from 0.1 to 1
Outputs:
- posed_vertices: bfloat16 [64, 3, 656], P(('vert', 'col'))
The draws below stay inside these ranges and needn't reach their ends.
Inputs may be any that keep to these rules, and one draw needn't show every extreme that they name: parents[0] = 0 and parents[j] < j for j >= 1. `skin_index`: the four joints of a vertex differ. `quaternions`: component 0 lies in [0.5, 1.5].
All inputs are finite; a program needn't handle non-finite values.
Results may differ from the reference program's by a relative error of at most 0.0024.
Values may be sent and summed in bfloat16 or wider, within the bound.
A program may use at most 64 MiB of HBM per device.

```python
import math
import jax
import jax.numpy as jnp
from jax import lax

K = 400
J = 55
V = 656
CHARS = 64
N_VERT = 8


def draw_quaternions(key, part):
    first_key = jax.random.fold_in(key, 11)
    second_key = jax.random.fold_in(key, 12)
    scalar_part = jax.random.uniform(first_key, (CHARS, 1, J), jnp.float32, 0.75, 1.25)
    vector_part = jnp.clip(0.4 * jax.random.normal(second_key, (CHARS, 3, J), jnp.float32), -1.5, 1.5)
    return jnp.concatenate([scalar_part, vector_part], axis=1)


def draw_parents(key, part):
    steps_back = jax.random.randint(jax.random.fold_in(key, 21), (J,), 0, 3)
    joint_ids = jnp.arange(J, dtype=jnp.int32)
    return jnp.maximum(joint_ids - 1 - steps_back, 0).astype(jnp.int32)


def level_of(own_key, shape, split, smallest, largest):
    factor_of = 1.0
    for dim, parts in split:
        draws = jax.random.uniform(jax.random.fold_in(jax.random.fold_in(own_key, 6), dim), (parts,), jnp.float32, smallest / len(split), largest / len(split))
        factor_of = factor_of * jnp.repeat(jnp.exp(draws), shape[dim] // parts).reshape((-1,) + (1,) * (len(shape) - 1 - dim))
    return factor_of


def picks_of(key, rows, count, top, lift):
    order = jax.random.permutation(jax.random.fold_in(key, 1), count)
    favour = order
    for power in range(3):
        favour = favour * favour // count
    favour = favour * lift // count
    tickets = jax.random.randint(jax.random.fold_in(key, 2), (rows, count), 0, 4096) + favour
    fixed_rows = jax.random.permutation(jax.random.fold_in(key, 3), rows)[jnp.arange(count) % rows]
    tickets = jnp.where(jnp.arange(rows)[:, None] == fixed_rows[None, :], 1 << 14, tickets)
    priority = tickets * count + jnp.arange(count)
    return lax.top_k(priority.astype(jnp.int32), top)[1].astype(jnp.int32)


def centred(own_key, shape, spread, bound, shards=(), kind=jnp.bfloat16):
    entries = spread * jax.random.normal(own_key, shape, jnp.float32)
    if shards:
        entries = entries * level_of(own_key, shape, shards, -0.22, 0.18)
    return jnp.clip(entries, -bound, bound).astype(kind)


def setup_inputs(seed: int = 0) -> dict:
    seeds = jax.random.split(jax.random.key(seed), 10)
    coeffs = centred(seeds[0], (CHARS, K), 1.0, 6.0, ((0, 32),))
    shape_basis = centred(seeds[1], (K, 3, V), K ** -0.5, 0.3125, ((0, 4), (2, 8)))
    template = centred(seeds[2], (3, V), 1.0, 6.0, ((1, 8),), jnp.float32)
    regressor = centred(seeds[3], (J, V), (V // 4) ** -0.5, 0.5, ((1, 8),), jnp.float32)
    quaternions = draw_quaternions(jax.random.fold_in(seeds[9], 71), 0)
    translation = centred(seeds[5], (CHARS, 3), 1.0, 6.0, ((0, 32),), jnp.float32)
    parents = draw_parents(jax.random.fold_in(seeds[9], 71), 0)
    skin_index = picks_of(seeds[7], V, J, 4, 595)
    skin_raw = jnp.clip(jnp.exp(math.log(1.0) - 2.3025851 * jax.random.uniform(seeds[8], (V, 4), jnp.float32) ** level_of(seeds[8], (V, 4), ((0, 8),), -0.2, 0.2)), 0.1, 1.0)
    return dict(coeffs=coeffs, shape_basis=shape_basis, template=template, regressor=regressor, quaternions=quaternions, translation=translation, parents=parents, skin_index=skin_index, skin_raw=skin_raw)


def rotations(quaternions):
    quat_w = jnp.transpose(quaternions[:, 0])
    quat_x = jnp.transpose(quaternions[:, 1])
    quat_y = jnp.transpose(quaternions[:, 2])
    quat_z = jnp.transpose(quaternions[:, 3])
    scale_two = 2.0 / (quat_w * quat_w + quat_x * quat_x + quat_y * quat_y + quat_z * quat_z)
    matrix_rows = [
        [1.0 - scale_two * (quat_y * quat_y + quat_z * quat_z), scale_two * (quat_x * quat_y - quat_w * quat_z), scale_two * (quat_x * quat_z + quat_w * quat_y)],
        [scale_two * (quat_x * quat_y + quat_w * quat_z), 1.0 - scale_two * (quat_x * quat_x + quat_z * quat_z), scale_two * (quat_y * quat_z - quat_w * quat_x)],
        [scale_two * (quat_x * quat_z - quat_w * quat_y), scale_two * (quat_y * quat_z + quat_w * quat_x), 1.0 - scale_two * (quat_x * quat_x + quat_y * quat_y)],
    ]
    return jnp.stack([jnp.stack(entry, axis=1) for entry in matrix_rows], axis=1)


def kinematics(joints, quaternions, translation, parents):
    joint_total = quaternions.shape[2]
    local_rots = rotations(quaternions)
    places = jnp.transpose(joints, (2, 1, 0))
    glob_rot = jnp.zeros_like(local_rots).at[0].set(local_rots[0])
    glob_pos = jnp.zeros_like(places).at[0].set(places[0] + jnp.transpose(translation))

    def compose(joint, state_pair):
        rot_now, pos_now = state_pair
        parent = lax.dynamic_index_in_dim(parents, joint, 0, keepdims=False)
        parent_rot = lax.dynamic_index_in_dim(rot_now, parent, 0, keepdims=False)
        parent_pos = lax.dynamic_index_in_dim(pos_now, parent, 0, keepdims=False)
        local_rot = lax.dynamic_index_in_dim(local_rots, joint, 0, keepdims=False)
        offset = lax.dynamic_index_in_dim(places, joint, 0, keepdims=False) - lax.dynamic_index_in_dim(places, parent, 0, keepdims=False)
        new_rot = jnp.einsum("amc,mbc->abc", parent_rot, local_rot, precision=lax.Precision.HIGHEST)
        new_pos = jnp.einsum("amc,mc->ac", parent_rot, offset, precision=lax.Precision.HIGHEST) + parent_pos
        rot_now = lax.dynamic_update_index_in_dim(rot_now, new_rot, joint, 0)
        pos_now = lax.dynamic_update_index_in_dim(pos_now, new_pos, joint, 0)
        return (rot_now, pos_now)

    glob_rot, glob_pos = lax.fori_loop(1, joint_total, compose, (glob_rot, glob_pos))
    correction = glob_pos - jnp.einsum("jamc,jmc->jac", glob_rot, places, precision=lax.Precision.HIGHEST)
    frames = jnp.concatenate([glob_rot.reshape(joint_total, 9, glob_rot.shape[3]), correction], axis=1)
    return jnp.transpose(frames, (2, 1, 0))


def dense_weights(joint_index, raw_weights, joint_total):
    shares = raw_weights / jnp.sum(raw_weights, axis=1, keepdims=True)
    matches = joint_index[None, :, :] == jnp.arange(joint_total, dtype=jnp.int32)[:, None, None]
    return jnp.sum(jnp.where(matches, shares[None, :, :], jnp.zeros_like(shares)[None, :, :]), axis=2)


def apply_frames(blended, shaped_wide):
    coords = []
    for axis_out in range(3):
        value = blended[:, 9 + axis_out]
        for axis_in in range(3):
            value = value + blended[:, 3 * axis_out + axis_in] * shaped_wide[:, axis_in]
        coords.append(value)
    return jnp.stack(coords, axis=1)


def reference(coeffs, shape_basis, template, regressor, quaternions, translation, parents, skin_index, skin_raw):
    components = shape_basis.shape[0]
    vert_total = shape_basis.shape[2]
    flat_basis = shape_basis.reshape(components, 3 * vert_total)
    base_row = template.reshape(1, 3 * vert_total)
    weight_grid = dense_weights(skin_index, skin_raw, J)
    basis_table = jnp.einsum("kmv,jv->kmj", shape_basis.astype(jnp.float32), regressor, precision=lax.Precision.HIGHEST)
    base_table = jnp.einsum("mv,jv->mj", template, regressor, precision=lax.Precision.HIGHEST)
    block_size = CHARS // N_VERT

    def block_pass(inputs):
        coeff_block, quat_block, shift_block = inputs
        shaped = (jnp.dot(coeff_block, flat_basis, preferred_element_type=jnp.float32) + base_row).astype(jnp.bfloat16)
        shaped_wide = shaped.reshape(block_size, 3, vert_total).astype(jnp.float32)
        joints = jnp.einsum("ck,kmj->cmj", coeff_block.astype(jnp.float32), basis_table, precision=lax.Precision.HIGHEST) + base_table[None]
        frames = kinematics(joints, quat_block, shift_block, parents)
        blended = jnp.einsum("cej,jv->cev", frames, weight_grid, precision=lax.Precision.HIGHEST)
        return apply_frames(blended, shaped_wide).astype(jnp.bfloat16)

    result = lax.map(block_pass, (coeffs.reshape(N_VERT, block_size, components), quaternions.reshape(N_VERT, block_size, 4, J), translation.reshape(N_VERT, block_size, 3)))
    return result.reshape(CHARS, 3, vert_total)
```

```python
import functools

import jax
import jax.numpy as jnp
from jax import lax
from jax.experimental import pallas as pl
from jax.experimental.pallas import tpu as pltpu
from jax.sharding import PartitionSpec as P

MESH = pl.DeviceIdType.MESH
LANES = 128
HALF = 64
SUB = 8
F32 = jnp.float32
BF16 = jnp.bfloat16
EXACT = lax.Precision.HIGHEST


def iota(shape, dim):
    return lax.broadcasted_iota(jnp.int32, shape, dim)


def dot(a, b, precision=None):
    return jnp.dot(a, b, precision=precision, preferred_element_type=F32)


def dot_nt(a, b, precision=None):
    return lax.dot_general(a, b, (((1,), (1,)), ((), ())), precision=precision, preferred_element_type=F32)


def each(count, step):
    if count <= 16:
        for k in range(1, count):
            step(k)
    else:

        def one(k, carry):
            step(k)
            return carry

        lax.fori_loop(1, count, one, 0)


def kernel(
    n_vert,
    n_col,
    parents_ref,
    coeffs_ref,
    basis_ref,
    template_ref,
    regressor_ref,
    quat_ref,
    shift_ref,
    index_ref,
    raw_ref,
    out_ref,
    msg,
    bas,
    part,
    sums_in,
    sent,
    got,
    reg_lo,
    reg_hi,
    state,
    diff,
    locals_ref,
    tree,
    msg_s,
    msg_r,
    bas_s,
    bas_r,
    part_s,
    part_r,
    pos_s,
    pos_r,
):
    me = lax.axis_index("vert")
    col = lax.axis_index("col")
    own = coeffs_ref.shape[0]
    comps = basis_ref.shape[2]
    block = basis_ref.shape[1]
    joints = regressor_ref.shape[0]
    group = min(n_vert, LANES // SUB)
    n_group = n_vert // group
    rows = group * SUB
    chars = group * own
    fold = chars // 2
    msg_rows = chars + fold

    barrier = pltpu.get_barrier_semaphore()

    def vert_peer(k):
        return (lax.rem(me + k, n_vert), col)

    def col_peer(k):
        return (me, lax.rem(col + k, n_col))

    each(n_vert, lambda k: pl.semaphore_signal(barrier, inc=1, device_id=vert_peer(k), device_id_type=MESH))
    each(n_col, lambda k: pl.semaphore_signal(barrier, inc=1, device_id=col_peer(k), device_id_type=MESH))

    msg[me] = jnp.zeros(msg.shape[1:], F32)
    for c in range(own):
        msg[me, 4 * c : 4 * c + 4, 0:joints] = quat_ref[c]
    coeff_rows = coeffs_ref[...].astype(F32)
    for kb in range(n_col):
        msg[me, SUB + own * kb : SUB + own * (kb + 1), 0:comps] = coeff_rows[:, kb * comps : (kb + 1) * comps]
    msg[me, 2 * SUB : 2 * SUB + own, 0:3] = shift_ref[...]
    bas[col] = basis_ref[...]

    reg_lo[...] = jnp.zeros(reg_lo.shape, F32)
    reg_hi[...] = jnp.zeros(reg_hi.shape, F32)
    reg_lo[0:joints, :] = regressor_ref[...]
    reg_hi[HALF : HALF + joints, :] = regressor_ref[...]
    sent[...] = jnp.zeros(sent.shape, F32)
    tree[...] = jnp.zeros(tree.shape, F32)
    state[...] = jnp.zeros(state.shape, F32)
    diff[...] = jnp.zeros(diff.shape, F32)
    lane8 = iota((SUB, LANES), 1)
    sub8 = iota((SUB, LANES), 0)
    axis_lane = jnp.minimum((lane8 % SUB) // own, 2)
    raw = raw_ref[...]
    shares = raw / jnp.sum(raw, axis=0, keepdims=True)
    joint_row = iota((HALF, block), 0)
    weights = jnp.zeros((HALF, block), F32)
    for i in range(index_ref.shape[0]):
        weights = weights + jnp.where(index_ref[i : i + 1, :] == joint_row, shares[i : i + 1, :], 0.0)

    pl.semaphore_wait(barrier, n_vert + n_col - 2)

    def copies(src, dst, send, recv, peer_of):
        def make(k):
            return pltpu.make_async_remote_copy(
                src_ref=src, dst_ref=dst, send_sem=send.at[k], recv_sem=recv.at[k], device_id=peer_of(k), device_id_type=MESH
            )

        return make

    msg_copy = copies(msg.at[me], msg.at[me], msg_s, msg_r, vert_peer)
    bas_copy = copies(basis_ref, bas.at[col], bas_s, bas_r, col_peer)
    each(n_vert, lambda k: msg_copy(k).start())
    each(n_col, lambda k: bas_copy(k).start())
    each(n_vert, lambda k: msg_copy(k).wait_recv())

    e_row = iota((chars + rows, rows), 0)
    e_col = iota((chars + rows, rows), 1)
    r_row = jnp.where(e_row < chars, 0, e_row - chars)
    source = jnp.where(e_row < chars, e_row // own, r_row // SUB)
    member = jnp.where(e_row < chars, e_row % own, r_row % own)
    coeff_blocks = []
    for g in range(n_group):
        table = msg[g * group : (g + 1) * group, SUB : 2 * SUB, :].reshape(rows, LANES).astype(BF16)
        picks = [(e_col == source * SUB + kb * own + member) for kb in range(n_col)]
        coeff_blocks.append([dot(p.astype(F32).astype(BF16), table).astype(BF16)[:, 0:comps] for p in picks])

    q_row = iota((LANES, rows), 0)
    q_col = iota((LANES, rows), 1)
    q_base = ((q_row // SUB) % group) * SUB + (q_row % own) * 4
    for g in range(n_group):
        quats = msg[g * group : (g + 1) * group, 0:SUB, :].reshape(rows, LANES)
        w, x, y, z = [
            jnp.transpose(dot((q_col == q_base + comp).astype(F32), quats, EXACT))[0:HALF] for comp in range(4)
        ]
        s = 2.0 / (w * w + x * x + y * y + z * z)
        matrix = [
            [1.0 - s * (y * y + z * z), s * (x * y - w * z), s * (x * z + w * y)],
            [s * (x * y + w * z), 1.0 - s * (x * x + z * z), s * (y * z - w * x)],
            [s * (x * z - w * y), s * (y * z + w * x), 1.0 - s * (x * x + y * y)],
        ]
        for m in range(3):
            for b in range(3):
                locals_ref[g, m, pl.ds(b, HALF, stride=SUB), :] = matrix[m][b]

    each(n_col, lambda k: bas_copy(k).wait_recv())
    shaped = []
    for g in range(n_group):
        full = []
        for m in range(3):
            total = template_ref[m : m + 1, :]
            for kb in range(n_col):
                total = total + dot_nt(coeff_blocks[g][kb], bas[kb, m])
            full.append(total)
        low = jnp.concatenate([full[0][0:chars], full[2][0:fold]], axis=0)
        high = jnp.concatenate([full[1][0:chars], full[2][fold:chars]], axis=0)
        part[g] = dot_nt(low, reg_lo[...], EXACT) + dot_nt(high, reg_hi[...], EXACT)
        shaped.append([f[chars:].astype(BF16).astype(F32) for f in full])

    part_copy = copies(part, sums_in.at[me], part_s, part_r, vert_peer)
    each(n_vert, lambda k: part_copy(k).start())
    sums_in[me] = part[...]

    def compose(j, g, above):
        at = pl.multiple_of(j * SUB, SUB)
        new = jnp.zeros((SUB, LANES), F32)
        for m in range(3):
            new = new + jnp.broadcast_to(above[m : m + 1, :], (SUB, LANES)) * locals_ref[g, m, pl.ds(at, SUB), :]
        mine = above + (lane8 % HALF == j).astype(F32)
        new = jnp.where(sub8 < 3, new, jnp.where(sub8 == 3, mine, 0.0))
        if isinstance(j, int):
            new = new + jnp.where((sub8 == 3) & (lane8 == joints), 1.0, 0.0)
        tree[g, j] = new
        state[g, pl.ds(at, SUB), :] = new
        diff[g, pl.ds(at, SUB), :] = above - new

    def descend(j, carry):
        for g in range(n_group):
            compose(j, g, tree[g, parents_ref[j]])
        return carry

    for g in range(n_group):
        compose(0, g, (axis_lane == sub8).astype(F32))
    lax.fori_loop(1, joints, descend, 0)

    def plane(ref, g, m):
        return ref[g, pl.ds(m, HALF, stride=SUB), :]

    weights_up = dot(jnp.transpose(plane(state, 0, 3)), weights, EXACT)
    lane = iota((rows, LANES), 1)
    row = iota((rows, LANES), 0)
    row_char = (row // SUB) * own + row % own
    row_axis = jnp.minimum((row % SUB) // own, 2)
    t_row = iota((rows, rows), 0)
    t_col = iota((rows, rows), 1)
    t_pick = (t_col == (t_row // SUB) * SUB + t_row % own).astype(F32)
    gains, turned, moved = [], [], []
    for g in range(n_group):
        gain = jnp.transpose(jnp.concatenate([plane(diff, g, 0), plane(diff, g, 1)], axis=0))[0:rows]
        last = jnp.concatenate([plane(diff, g, 2)] * 2, axis=0)
        last = jnp.transpose(last)[0:rows]
        last = jnp.where((lane < HALF) == (row_char < fold), last, 0.0)
        gains.append((gain, last))
        shift = dot(t_pick, msg[g * group : (g + 1) * group, 2 * SUB : 3 * SUB, :].reshape(rows, LANES), EXACT)
        shift = jnp.sum(jnp.where(lane == row_axis, shift, 0.0), axis=1, keepdims=True)
        moved.append(jnp.where(lane == joints, shift, 0.0))
        turn = jnp.zeros((rows, block), F32)
        for m in range(3):
            if m == 0:
                pair = jnp.transpose(jnp.concatenate([plane(state, g, 0), plane(state, g, 1)], axis=0))[0:rows]
                spun = pair[:, 0:HALF]
            elif m == 1:
                spun = pair[:, HALF:LANES]
            else:
                spun = jnp.transpose(jnp.concatenate([plane(state, g, 2)] * 2, axis=0))[0:rows, 0:HALF]
            turn = turn + dot(spun, weights, EXACT) * shaped[g][m]
        turned.append(turn)

    x_row = iota((2 * rows, msg_rows), 0)
    x_col = iota((2 * rows, msg_rows), 1)
    x_r = x_row % rows
    x_char = (x_r // SUB) * own + x_r % own
    spread = (x_col == jnp.where(x_row < rows, x_char, chars + x_char % fold)).astype(F32)
    each(n_vert, lambda k: part_copy(k).wait_recv())
    for g in range(n_group):
        if n_vert <= 16:
            summed = sums_in[0, g]
            for i in range(1, n_vert):
                summed = summed + sums_in[i, g]
        else:
            summed = lax.fori_loop(1, n_vert, lambda i, a: a + sums_in[i, g], sums_in[0, g])
        wide = dot(spread, summed, EXACT)
        term = gains[g][0] * wide[0:rows] + gains[g][1] * wide[rows:] + moved[g]
        posed = turned[g] + dot(term, weights_up, EXACT)
        sent[g * group : (g + 1) * group, :, 0:block] = posed.reshape(group, SUB, block)

    def pos_copy(k):
        target = lax.rem(me + k, n_vert)
        return pltpu.make_async_remote_copy(
            src_ref=sent.at[target],
            dst_ref=got.at[me],
            send_sem=pos_s.at[k],
            recv_sem=pos_r.at[k],
            device_id=(target, col),
            device_id_type=MESH,
        )

    each(n_vert, lambda k: pos_copy(k).start())
    got[me] = sent[me]
    each(n_vert, lambda k: pos_copy(k).wait_recv())

    n_cols = -(-n_vert * block // LANES) + 1
    columns = [None] * n_cols

    def put(q, value):
        columns[q] = value if columns[q] is None else columns[q] + value

    for i in range(n_vert):
        q, r = divmod(i * block, LANES)
        tile = got[i]
        if r:
            tile = pltpu.roll(tile, r, 1)
        if r + block > LANES:
            put(q, jnp.where(lane8 >= r, tile, 0.0))
            put(q + 1, jnp.where(lane8 < r, tile, 0.0))
        else:
            put(q, tile)
    width = n_vert * block
    for q in range(n_cols):
        size = min(LANES, width - q * LANES)
        if size > 0:
            value = columns[q].astype(BF16)
            for a in range(3):
                out_ref[a, :, q * LANES : q * LANES + size] = value[own * a : own * (a + 1), 0:size]

    each(n_vert, lambda k: msg_copy(k).wait_send())
    each(n_col, lambda k: bas_copy(k).wait_send())
    each(n_vert, lambda k: part_copy(k).wait_send())
    each(n_vert, lambda k: pos_copy(k).wait_send())


def body(n_vert, n_col, coeffs, shape_basis, template, regressor, quaternions, translation, parents, skin_index, skin_raw):
    own = coeffs.shape[0]
    comps, _, block = shape_basis.shape
    joints = regressor.shape[0]
    group = min(n_vert, LANES // SUB)
    n_group = n_vert // group
    msg_rows = group * own + group * own // 2
    vmem = pl.BlockSpec(memory_space=pltpu.VMEM)
    dma = pltpu.SemaphoreType.DMA
    out = pl.pallas_call(
        functools.partial(kernel, n_vert, n_col),
        out_shape=jax.ShapeDtypeStruct((3, own, n_vert * block), BF16),
        in_specs=[pl.BlockSpec(memory_space=pltpu.SMEM)] + [vmem] * 8,
        out_specs=vmem,
        scratch_shapes=[
            pltpu.VMEM((n_vert, 3 * SUB, LANES), F32),
            pltpu.VMEM((n_col, 3, block, comps), BF16),
            pltpu.VMEM((n_group, msg_rows, LANES), F32),
            pltpu.VMEM((n_vert, n_group, msg_rows, LANES), F32),
            pltpu.VMEM((n_vert, SUB, LANES), F32),
            pltpu.VMEM((n_vert, SUB, LANES), F32),
            pltpu.VMEM((LANES, block), F32),
            pltpu.VMEM((LANES, block), F32),
            pltpu.VMEM((n_group, HALF * SUB, LANES), F32),
            pltpu.VMEM((n_group, HALF * SUB, LANES), F32),
            pltpu.VMEM((n_group, 3, HALF * SUB, LANES), F32),
            pltpu.VMEM((n_group, joints, SUB, LANES), F32),
            dma((n_vert,)),
            dma((n_vert,)),
            dma((n_col,)),
            dma((n_col,)),
            dma((n_vert,)),
            dma((n_vert,)),
            dma((n_vert,)),
            dma((n_vert,)),
        ],
        compiler_params=pltpu.CompilerParams(collective_id=0, has_side_effects=True),
    )(
        parents,
        coeffs,
        jnp.transpose(shape_basis, (1, 2, 0)),
        template,
        regressor,
        quaternions,
        translation,
        jnp.transpose(skin_index),
        jnp.transpose(skin_raw),
    )
    return jnp.transpose(out, (1, 0, 2))


def solution(mesh):
    in_specs = (
        P(("vert", "col"), None),
        P("col", None, "vert"),
        P(None, "vert"),
        P(None, "vert"),
        P(("vert", "col"), None, None),
        P(("vert", "col"), None),
        P(),
        P("vert", None),
        P("vert", None),
    )
    out_specs = P(("vert", "col"), None, None)
    step = functools.partial(body, mesh.shape["vert"], mesh.shape["col"])
    return jax.shard_map(step, mesh=mesh, in_specs=in_specs, out_specs=out_specs, check_vma=False)
```

```python
import functools

import jax
import jax.numpy as jnp
from jax import lax
from jax.experimental import pallas as pl
from jax.experimental.pallas import tpu as pltpu
from jax.sharding import PartitionSpec as P

MESH = pl.DeviceIdType.MESH
LANES = 128
HALF = 64
SUB = 8
F32 = jnp.float32
BF16 = jnp.bfloat16
EXACT = lax.Precision.HIGHEST


def iota(shape, dim):
    return lax.broadcasted_iota(jnp.int32, shape, dim)


def dot(a, b, precision=None):
    return jnp.dot(a, b, precision=precision, preferred_element_type=F32)


def dot_nt(a, b, precision=None):
    return lax.dot_general(a, b, (((1,), (1,)), ((), ())), precision=precision, preferred_element_type=F32)


def each(count, step):
    if count <= 16:
        for k in range(1, count):
            step(k)
    else:

        def one(k, carry):
            step(k)
            return carry

        lax.fori_loop(1, count, one, 0)


def kernel(
    n_vert,
    n_col,
    parents_hbm,
    coeffs_hbm,
    basis_hbm,
    template_hbm,
    regressor_hbm,
    quat_hbm,
    shift_hbm,
    index_hbm,
    raw_hbm,
    out_ref,
    parents,
    coeff_in,
    bas,
    template,
    regressor,
    quat,
    shift,
    index_in,
    raw_in,
    quat_rows,
    coeff_rows,
    sent,
    got,
    tree,
    state,
    diff,
    locals_ref,
    weights,
    local_s,
    coeff_s,
    coeff_r,
    bas_s,
    bas_r,
    index_s,
    index_r,
    raw_s,
    raw_r,
    sent_s,
    sent_r,
):
    me = lax.axis_index("vert")
    col = lax.axis_index("col")
    own, _ = coeffs_hbm.shape
    _, block, comps = basis_hbm.shape
    joints = regressor_hbm.shape[0]
    rows = n_vert * SUB

    barrier = pltpu.get_barrier_semaphore()

    def vert_peer(k):
        return (lax.rem(me + k, n_vert), col)

    def col_peer(k):
        return (me, lax.rem(col + k, n_col))

    each(n_vert, lambda k: pl.semaphore_signal(barrier, inc=1, device_id=vert_peer(k), device_id_type=MESH))
    each(n_col, lambda k: pl.semaphore_signal(barrier, inc=1, device_id=col_peer(k), device_id_type=MESH))

    pairs = [
        (coeffs_hbm, coeff_in.at[me]),
        (basis_hbm, bas.at[col]),
        (index_hbm, index_in.at[me]),
        (raw_hbm, raw_in.at[me]),
        (parents_hbm, parents),
        (quat_hbm, quat),
        (shift_hbm, shift),
        (template_hbm, template),
        (regressor_hbm, regressor),
    ]
    loads = [pltpu.make_async_copy(src, dst, local_s.at[i]) for i, (src, dst) in enumerate(pairs)]
    for load in loads:
        load.start()

    sub8 = iota((SUB, LANES), 0)
    lane8 = iota((SUB, LANES), 1)
    axis_lane = jnp.minimum((lane8 % SUB) // own, 2)
    quat_rows[...] = jnp.zeros(quat_rows.shape, F32)
    weights[...] = jnp.zeros(weights.shape, F32)
    tree[...] = jnp.zeros(tree.shape, F32)
    state[...] = jnp.zeros(state.shape, F32)
    diff[...] = jnp.zeros(diff.shape, F32)
    sent[...] = jnp.zeros(sent.shape, F32)
    for load in loads:
        load.wait()

    def copies(src, dst, send, recv, peer_of):
        def make(k):
            return pltpu.make_async_remote_copy(
                src_ref=src, dst_ref=dst, send_sem=send.at[k], recv_sem=recv.at[k], device_id=peer_of(k), device_id_type=MESH
            )

        return make

    coeff_copy = copies(coeff_in.at[me], coeff_in.at[me], coeff_s, coeff_r, vert_peer)
    bas_copy = copies(bas.at[col], bas.at[col], bas_s, bas_r, col_peer)
    index_copy = copies(index_in.at[me], index_in.at[me], index_s, index_r, vert_peer)
    raw_copy = copies(raw_in.at[me], raw_in.at[me], raw_s, raw_r, vert_peer)

    pl.semaphore_wait(barrier, n_vert + n_col - 2)
    each(n_vert, lambda k: coeff_copy(k).start())
    each(n_col, lambda k: bas_copy(k).start())
    each(n_vert, lambda k: index_copy(k).start())
    each(n_vert, lambda k: raw_copy(k).start())

    for c in range(own):
        quat_rows[4 * c : 4 * c + 4, 0:joints] = quat[c]
    q_row = iota((LANES, SUB), 0)
    q_col = iota((LANES, SUB), 1)
    w, x, y, z = [
        jnp.transpose(dot((q_col == (q_row % own) * 4 + comp).astype(F32), quat_rows[...], EXACT))[0:HALF] for comp in range(4)
    ]
    s = 2.0 / (w * w + x * x + y * y + z * z)
    matrix = [
        [1.0 - s * (y * y + z * z), s * (x * y - w * z), s * (x * z + w * y)],
        [s * (x * y + w * z), 1.0 - s * (x * x + z * z), s * (y * z - w * x)],
        [s * (x * z - w * y), s * (y * z + w * x), 1.0 - s * (x * x + y * y)],
    ]
    for m in range(3):
        for b in range(3):
            locals_ref[m, pl.ds(b, HALF, stride=SUB), :] = matrix[m][b]

    def compose(j, above):
        at = pl.multiple_of(j * SUB, SUB)
        new = jnp.zeros((SUB, LANES), F32)
        for m in range(3):
            new = new + jnp.broadcast_to(above[m : m + 1, :], (SUB, LANES)) * locals_ref[m, pl.ds(at, SUB), :]
        mine = above + (lane8 % HALF == j).astype(F32)
        new = jnp.where(sub8 < 3, new, jnp.where(sub8 == 3, mine, 0.0))
        if isinstance(j, int):
            new = new + jnp.where((sub8 == 3) & (lane8 == joints), 1.0, 0.0)
        tree[j] = new
        state[pl.ds(at, SUB), :] = new
        diff[pl.ds(at, SUB), :] = above - new

    def descend(j, carry):
        compose(j, tree[parents[j]])
        return carry

    compose(0, (axis_lane == sub8).astype(F32))
    lax.fori_loop(1, joints, descend, 0)

    def flipped(ref, m, n):
        value = ref[pl.ds(m, HALF, stride=SUB), :]
        return jnp.transpose(jnp.concatenate([value, value], axis=0))[0:n]

    gains = [flipped(diff, m, SUB) for m in range(3)]
    gains = [jnp.where(lane8 < HALF, gain, 0.0) for gain in gains]
    factors = jnp.concatenate(
        [flipped(state, m, SUB)[:, 0:HALF] for m in range(3)] + [flipped(state, 3, HALF)[:, 0:HALF]], axis=0
    )
    moves = jnp.concatenate([shift[...]] * (SUB // own), axis=0)
    m_axis = jnp.minimum(iota(moves.shape, 0) // own, 2)
    moves = jnp.sum(jnp.where(iota(moves.shape, 1) == m_axis, moves, 0.0), axis=1, keepdims=True)
    moves = jnp.where(lane8 == joints, moves, 0.0)

    each(n_vert, lambda k: coeff_copy(k).wait_recv())
    for i in range(n_vert):
        one = coeff_in[i].astype(F32)
        coeff_rows[i * SUB : (i + 1) * SUB, 0 : n_col * comps] = jnp.concatenate([one] * (SUB // own), axis=0)
    blocks = [coeff_rows[:, kb * comps : (kb + 1) * comps].astype(BF16) for kb in range(n_col)]

    each(n_col, lambda k: bas_copy(k).wait_recv())
    r_axis = jnp.minimum((iota((rows, block), 0) % SUB) // own, 2)
    full = jnp.zeros((rows, block), F32)
    for m in range(3):
        total = template[m : m + 1, :]
        for kb in range(n_col):
            total = total + dot_nt(blocks[kb], bas[kb, m])
        full = jnp.where(r_axis == m, total, full)
    share = dot_nt(full, regressor[...], EXACT)
    sent[:, 0, :, 0:block] = full.astype(BF16).astype(F32).reshape(n_vert, SUB, block)
    sent[:, 1, :, 0:joints] = share.reshape(n_vert, SUB, joints)

    def sent_copy(k):
        target = lax.rem(me + k, n_vert)
        return pltpu.make_async_remote_copy(
            src_ref=sent.at[target],
            dst_ref=got.at[me],
            send_sem=sent_s.at[k],
            recv_sem=sent_r.at[k],
            device_id=(target, col),
            device_id_type=MESH,
        )

    each(n_vert, lambda k: sent_copy(k).start())
    got[me] = sent[me]

    each(n_vert, lambda k: index_copy(k).wait_recv())
    each(n_vert, lambda k: raw_copy(k).wait_recv())
    joint_row = iota((HALF, block), 0)
    for i in range(n_vert):
        raw = raw_in[i]
        raw = raw / jnp.sum(raw, axis=0, keepdims=True)
        index = index_in[i]
        grid = jnp.zeros((HALF, block), F32)
        for slot in range(raw.shape[0]):
            grid = jnp.where(index[slot : slot + 1, :] == joint_row, raw[slot : slot + 1, :], grid)
        weights[:, i * LANES : i * LANES + block] = grid
    blended = dot(factors, weights[...], EXACT)
    turns = [blended[m * SUB : (m + 1) * SUB] for m in range(3)]
    upper = blended[3 * SUB :]
    upper_hi = upper.astype(BF16)
    upper_lo = (upper - upper_hi.astype(F32)).astype(BF16)
    upper_all = jnp.concatenate([upper_hi, upper_lo, upper_hi], axis=0)

    def rows_of(tile):
        spun = [tile] + [pltpu.roll(tile, own * q, 0) for q in range(1, SUB // own)]
        count = SUB // own
        result = []
        for m in range(3):
            value = spun[(-m) % count]
            for q in range(1, count):
                value = jnp.where(sub8 // own == q, spun[(q - m) % count], value)
            result.append(value)
        return result

    each(n_vert, lambda k: sent_copy(k).wait_recv())
    summed = got[0, 1]
    for i in range(1, n_vert):
        summed = summed + got[i, 1]
    places = rows_of(summed)
    term = moves
    for m in range(3):
        term = term + gains[m] * places[m]
    term_hi = term.astype(BF16)
    term_lo = (term - term_hi.astype(F32)).astype(BF16)
    term_all = jnp.concatenate([term_hi[:, 0:HALF], term_hi[:, 0:HALF], term_lo[:, 0:HALF]], axis=1)
    moved = dot(term_all, upper_all)

    n_cols = -(-n_vert * block // LANES) + 1
    columns = [None] * n_cols

    def put(q, value):
        columns[q] = value if columns[q] is None else columns[q] + value

    for i in range(n_vert):
        q, r = divmod(i * block, LANES)
        at = slice(i * LANES, (i + 1) * LANES)
        shaped = rows_of(got[i, 0])
        tile = moved[:, at]
        for m in range(3):
            tile = tile + turns[m][:, at] * shaped[m]
        if r:
            tile = pltpu.roll(tile, r, 1)
        if r + block > LANES:
            put(q, jnp.where(lane8 >= r, tile, 0.0))
            put(q + 1, jnp.where(lane8 < r, tile, 0.0))
        else:
            put(q, tile)
    width = n_vert * block
    for q in range(n_cols):
        size = min(LANES, width - q * LANES)
        if size > 0:
            value = columns[q].astype(out_ref.dtype)
            for a in range(3):
                out_ref[a, :, q * LANES : q * LANES + size] = value[own * a : own * (a + 1), 0:size]

    each(n_vert, lambda k: coeff_copy(k).wait_send())
    each(n_col, lambda k: bas_copy(k).wait_send())
    each(n_vert, lambda k: index_copy(k).wait_send())
    each(n_vert, lambda k: raw_copy(k).wait_send())
    each(n_vert, lambda k: sent_copy(k).wait_send())


def body(n_vert, n_col, coeffs, shape_basis, template, regressor, quaternions, translation, parents, skin_index, skin_raw):
    own, total = coeffs.shape
    comps, _, block = shape_basis.shape
    joints = regressor.shape[0]
    slots = skin_index.shape[1]
    vmem = pl.BlockSpec(memory_space=pltpu.VMEM)
    anywhere = pl.BlockSpec(memory_space=pl.ANY)
    dma = pltpu.SemaphoreType.DMA
    out = pl.pallas_call(
        functools.partial(kernel, n_vert, n_col),
        out_shape=jax.ShapeDtypeStruct((3, own, n_vert * block), BF16),
        in_specs=[anywhere] * 9,
        out_specs=vmem,
        scratch_shapes=[
            pltpu.SMEM((joints,), jnp.int32),
            pltpu.VMEM((n_vert, own, total), BF16),
            pltpu.VMEM((n_col, 3, block, comps), BF16),
            pltpu.VMEM((3, block), F32),
            pltpu.VMEM((joints, block), F32),
            pltpu.VMEM((own, 4, joints), F32),
            pltpu.VMEM((own, 3), F32),
            pltpu.VMEM((n_vert, slots, block), jnp.int32),
            pltpu.VMEM((n_vert, slots, block), F32),
            pltpu.VMEM((SUB, LANES), F32),
            pltpu.VMEM((n_vert * SUB, total), F32),
            pltpu.VMEM((n_vert, 2, SUB, LANES), F32),
            pltpu.VMEM((n_vert, 2, SUB, LANES), F32),
            pltpu.VMEM((joints, SUB, LANES), F32),
            pltpu.VMEM((HALF * SUB, LANES), F32),
            pltpu.VMEM((HALF * SUB, LANES), F32),
            pltpu.VMEM((3, HALF * SUB, LANES), F32),
            pltpu.VMEM((HALF, n_vert * LANES), F32),
            dma((9,)),
            dma((n_vert,)),
            dma((n_vert,)),
            dma((n_col,)),
            dma((n_col,)),
            dma((n_vert,)),
            dma((n_vert,)),
            dma((n_vert,)),
            dma((n_vert,)),
            dma((n_vert,)),
            dma((n_vert,)),
        ],
        compiler_params=pltpu.CompilerParams(collective_id=0, has_side_effects=True),
    )(
        parents,
        coeffs,
        jnp.transpose(shape_basis, (1, 2, 0)),
        template,
        regressor,
        quaternions,
        translation,
        jnp.transpose(skin_index),
        jnp.transpose(skin_raw),
    )
    return jnp.transpose(out, (1, 0, 2))


def solution(mesh):
    in_specs = (
        P(("vert", "col"), None),
        P("col", None, "vert"),
        P(None, "vert"),
        P(None, "vert"),
        P(("vert", "col"), None, None),
        P(("vert", "col"), None),
        P(),
        P("vert", None),
        P("vert", None),
    )
    out_specs = P(("vert", "col"), None, None)
    step = functools.partial(body, mesh.shape["vert"], mesh.shape["col"])
    return jax.shard_map(step, mesh=mesh, in_specs=in_specs, out_specs=out_specs, check_vma=False)
```

```python
import functools

import jax
import jax.numpy as jnp
from jax import lax
from jax.experimental import pallas as pl
from jax.experimental.pallas import tpu as pltpu
from jax.sharding import PartitionSpec as P

MESH = pl.DeviceIdType.MESH
LANES = 128
HALF = 64
SUB = 8
F32 = jnp.float32
BF16 = jnp.bfloat16
EXACT = lax.Precision.HIGHEST


def iota(shape, dim):
    return lax.broadcasted_iota(jnp.int32, shape, dim)


def dot(a, b, precision=None):
    return jnp.dot(a, b, precision=precision, preferred_element_type=F32)


def dot_nt(a, b, precision=None):
    return lax.dot_general(a, b, (((1,), (1,)), ((), ())), precision=precision, preferred_element_type=F32)


def each(count, step):
    if count <= 16:
        for k in range(1, count):
            step(k)
    else:

        def one(k, carry):
            step(k)
            return carry

        lax.fori_loop(1, count, one, 0)


def kernel(
    n_vert,
    n_col,
    parents_hbm,
    coeffs_hbm,
    basis_hbm,
    template_hbm,
    regressor_hbm,
    quat_hbm,
    shift_hbm,
    index_hbm,
    raw_hbm,
    out_ref,
    parents,
    coeff_in,
    bas,
    template,
    regressor,
    quat,
    shift,
    index_in,
    raw_in,
    quat_rows,
    coeff_rows,
    blocks,
    sent,
    got,
    tree,
    state,
    diff,
    locals_ref,
    weights,
    local_s,
    coeff_s,
    coeff_r,
    bas_s,
    bas_r,
    index_s,
    index_r,
    raw_s,
    raw_r,
    sent_s,
    sent_r,
):
    me = lax.axis_index("vert")
    col = lax.axis_index("col")
    own, _ = coeffs_hbm.shape
    _, block, comps = basis_hbm.shape
    joints = regressor_hbm.shape[0]
    rows = n_vert * SUB

    barrier = pltpu.get_barrier_semaphore()

    def vert_peer(k):
        return (lax.rem(me + k, n_vert), col)

    def col_peer(k):
        return (me, lax.rem(col + k, n_col))

    each(n_vert, lambda k: pl.semaphore_signal(barrier, inc=1, device_id=vert_peer(k), device_id_type=MESH))
    each(n_col, lambda k: pl.semaphore_signal(barrier, inc=1, device_id=col_peer(k), device_id_type=MESH))

    pairs = [
        (coeffs_hbm, coeff_in.at[me]),
        (basis_hbm, bas.at[col]),
        (index_hbm, index_in.at[me]),
        (raw_hbm, raw_in.at[me]),
        (parents_hbm, parents),
        (quat_hbm, quat),
        (shift_hbm, shift),
        (template_hbm, template),
        (regressor_hbm, regressor),
    ]
    loads = [pltpu.make_async_copy(src, dst, local_s.at[i]) for i, (src, dst) in enumerate(pairs)]
    for load in loads:
        load.start()

    sub8 = iota((SUB, LANES), 0)
    lane8 = iota((SUB, LANES), 1)
    axis_lane = jnp.minimum((lane8 % SUB) // own, 2)
    quat_rows[...] = jnp.zeros(quat_rows.shape, F32)
    weights[...] = jnp.zeros(weights.shape, F32)
    tree[...] = jnp.zeros(tree.shape, F32)
    state[...] = jnp.zeros(state.shape, F32)
    diff[...] = jnp.zeros(diff.shape, F32)
    sent[...] = jnp.zeros(sent.shape, F32)
    for load in loads:
        load.wait()

    def copies(src, dst, send, recv, peer_of):
        def make(k):
            return pltpu.make_async_remote_copy(
                src_ref=src, dst_ref=dst, send_sem=send.at[k], recv_sem=recv.at[k], device_id=peer_of(k), device_id_type=MESH
            )

        return make

    coeff_copy = copies(coeff_in.at[me], coeff_in.at[me], coeff_s, coeff_r, vert_peer)
    bas_copy = copies(bas.at[col], bas.at[col], bas_s, bas_r, col_peer)
    index_copy = copies(index_in.at[me], index_in.at[me], index_s, index_r, vert_peer)
    raw_copy = copies(raw_in.at[me], raw_in.at[me], raw_s, raw_r, vert_peer)

    pl.semaphore_wait(barrier, n_vert + n_col - 2)
    each(n_col, lambda k: bas_copy(k).start())
    each(n_vert, lambda k: coeff_copy(k).start())
    each(n_vert, lambda k: index_copy(k).start())
    each(n_vert, lambda k: raw_copy(k).start())

    for c in range(own):
        quat_rows[4 * c : 4 * c + 4, 0:joints] = quat[c]
    q_row = iota((LANES, SUB), 0)
    q_col = iota((LANES, SUB), 1)
    w, x, y, z = [
        jnp.transpose(dot((q_col == (q_row % own) * 4 + comp).astype(F32), quat_rows[...], EXACT))[0:HALF] for comp in range(4)
    ]
    s = 2.0 / (w * w + x * x + y * y + z * z)
    matrix = [
        [1.0 - s * (y * y + z * z), s * (x * y - w * z), s * (x * z + w * y)],
        [s * (x * y + w * z), 1.0 - s * (x * x + z * z), s * (y * z - w * x)],
        [s * (x * z - w * y), s * (y * z + w * x), 1.0 - s * (x * x + y * y)],
    ]
    for m in range(3):
        for b in range(3):
            locals_ref[m, pl.ds(b, HALF, stride=SUB), :] = matrix[m][b]

    def compose(j, above):
        at = pl.multiple_of(j * SUB, SUB)
        new = jnp.zeros((SUB, LANES), F32)
        for m in range(3):
            new = new + jnp.broadcast_to(above[m : m + 1, :], (SUB, LANES)) * locals_ref[m, pl.ds(at, SUB), :]
        mine = above + (lane8 % HALF == j).astype(F32)
        new = jnp.where(sub8 < 3, new, jnp.where(sub8 == 3, mine, 0.0))
        if isinstance(j, int):
            new = new + jnp.where((sub8 == 3) & (lane8 == joints), 1.0, 0.0)
        tree[j] = new
        state[pl.ds(at, SUB), :] = new
        diff[pl.ds(at, SUB), :] = above - new

    def descend(j, carry):
        compose(j, tree[parents[j]])
        return carry

    compose(0, (axis_lane == sub8).astype(F32))
    lax.fori_loop(1, joints, descend, 0)

    def flipped(ref, m, n):
        value = ref[pl.ds(m, HALF, stride=SUB), :]
        return jnp.transpose(jnp.concatenate([value, value], axis=0))[0:n]

    gains = [flipped(diff, m, SUB) for m in range(3)]
    gains = [jnp.where(lane8 < HALF, gain, 0.0) for gain in gains]
    factors = jnp.concatenate(
        [flipped(state, m, SUB)[:, 0:HALF] for m in range(3)] + [flipped(state, 3, HALF)[:, 0:HALF]], axis=0
    )
    moves = jnp.concatenate([shift[...]] * (SUB // own), axis=0)
    m_axis = jnp.minimum(iota(moves.shape, 0) // own, 2)
    moves = jnp.sum(jnp.where(iota(moves.shape, 1) == m_axis, moves, 0.0), axis=1, keepdims=True)
    moves = jnp.where(lane8 == joints, moves, 0.0)

    each(n_vert, lambda k: coeff_copy(k).wait_recv())
    for i in range(n_vert):
        one = coeff_in[i].astype(F32)
        coeff_rows[i * SUB : (i + 1) * SUB, 0 : n_col * comps] = jnp.concatenate([one] * (SUB // own), axis=0)
    for kb in range(n_col):
        blocks[kb] = coeff_rows[:, kb * comps : (kb + 1) * comps].astype(BF16)

    totals = [template[m : m + 1, :] + dot_nt(blocks[col], bas[col, m]) for m in range(3)]
    for k in range(1, n_col):
        bas_copy(k).wait_recv()
        source = lax.rem(col + n_col - k, n_col)
        totals = [totals[m] + dot_nt(blocks[source], bas[source, m]) for m in range(3)]
    r_axis = jnp.minimum((iota((rows, block), 0) % SUB) // own, 2)
    full = jnp.where(r_axis == 0, totals[0], jnp.where(r_axis == 1, totals[1], totals[2]))
    share = dot_nt(full, regressor[...], EXACT)
    sent[:, 0, :, 0:block] = full.astype(BF16).astype(F32).reshape(n_vert, SUB, block)
    sent[:, 1, :, 0:joints] = share.reshape(n_vert, SUB, joints)

    def sent_copy(k):
        target = lax.rem(me + k, n_vert)
        return pltpu.make_async_remote_copy(
            src_ref=sent.at[target],
            dst_ref=got.at[me],
            send_sem=sent_s.at[k],
            recv_sem=sent_r.at[k],
            device_id=(target, col),
            device_id_type=MESH,
        )

    each(n_vert, lambda k: sent_copy(k).start())
    got[me] = sent[me]

    each(n_vert, lambda k: index_copy(k).wait_recv())
    each(n_vert, lambda k: raw_copy(k).wait_recv())
    joint_row = iota((HALF, block), 0)
    for i in range(n_vert):
        raw = raw_in[i]
        raw = raw / jnp.sum(raw, axis=0, keepdims=True)
        index = index_in[i]
        grid = jnp.zeros((HALF, block), F32)
        for slot in range(raw.shape[0]):
            grid = jnp.where(index[slot : slot + 1, :] == joint_row, raw[slot : slot + 1, :], grid)
        weights[:, i * LANES : i * LANES + block] = grid
    blended = dot(factors, weights[...], EXACT)
    turns = [blended[m * SUB : (m + 1) * SUB] for m in range(3)]
    upper = blended[3 * SUB :]
    upper_hi = upper.astype(BF16)
    upper_lo = (upper - upper_hi.astype(F32)).astype(BF16)
    upper_all = jnp.concatenate([upper_hi, upper_lo, upper_hi], axis=0)

    def rows_of(tile):
        spun = [tile] + [pltpu.roll(tile, own * q, 0) for q in range(1, SUB // own)]
        count = SUB // own
        result = []
        for m in range(3):
            value = spun[(-m) % count]
            for q in range(1, count):
                value = jnp.where(sub8 // own == q, spun[(q - m) % count], value)
            result.append(value)
        return result

    each(n_vert, lambda k: sent_copy(k).wait_recv())
    summed = got[0, 1]
    for i in range(1, n_vert):
        summed = summed + got[i, 1]
    places = rows_of(summed)
    term = moves
    for m in range(3):
        term = term + gains[m] * places[m]
    term_hi = term.astype(BF16)
    term_lo = (term - term_hi.astype(F32)).astype(BF16)
    term_all = jnp.concatenate([term_hi[:, 0:HALF], term_hi[:, 0:HALF], term_lo[:, 0:HALF]], axis=1)
    moved = dot(term_all, upper_all)

    n_cols = -(-n_vert * block // LANES) + 1
    columns = [None] * n_cols

    def put(q, value):
        columns[q] = value if columns[q] is None else columns[q] + value

    for i in range(n_vert):
        q, r = divmod(i * block, LANES)
        at = slice(i * LANES, (i + 1) * LANES)
        shaped = rows_of(got[i, 0])
        tile = moved[:, at]
        for m in range(3):
            tile = tile + turns[m][:, at] * shaped[m]
        if r:
            tile = pltpu.roll(tile, r, 1)
        if r + block > LANES:
            put(q, jnp.where(lane8 >= r, tile, 0.0))
            put(q + 1, jnp.where(lane8 < r, tile, 0.0))
        else:
            put(q, tile)
    width = n_vert * block
    for q in range(n_cols):
        size = min(LANES, width - q * LANES)
        if size > 0:
            value = columns[q].astype(out_ref.dtype)
            for a in range(3):
                out_ref[a, :, q * LANES : q * LANES + size] = value[own * a : own * (a + 1), 0:size]

    each(n_vert, lambda k: coeff_copy(k).wait_send())
    each(n_col, lambda k: bas_copy(k).wait_send())
    each(n_vert, lambda k: index_copy(k).wait_send())
    each(n_vert, lambda k: raw_copy(k).wait_send())
    each(n_vert, lambda k: sent_copy(k).wait_send())


def body(n_vert, n_col, coeffs, shape_basis, template, regressor, quaternions, translation, parents, skin_index, skin_raw):
    own, total = coeffs.shape
    comps, _, block = shape_basis.shape
    joints = regressor.shape[0]
    slots = skin_index.shape[1]
    vmem = pl.BlockSpec(memory_space=pltpu.VMEM)
    anywhere = pl.BlockSpec(memory_space=pl.ANY)
    dma = pltpu.SemaphoreType.DMA
    out = pl.pallas_call(
        functools.partial(kernel, n_vert, n_col),
        out_shape=jax.ShapeDtypeStruct((3, own, n_vert * block), F32),
        in_specs=[anywhere] * 9,
        out_specs=vmem,
        scratch_shapes=[
            pltpu.SMEM((joints,), jnp.int32),
            pltpu.VMEM((n_vert, own, total), BF16),
            pltpu.VMEM((n_col, 3, block, comps), BF16),
            pltpu.VMEM((3, block), F32),
            pltpu.VMEM((joints, block), F32),
            pltpu.VMEM((own, 4, joints), F32),
            pltpu.VMEM((own, 3), F32),
            pltpu.VMEM((n_vert, slots, block), jnp.int32),
            pltpu.VMEM((n_vert, slots, block), F32),
            pltpu.VMEM((SUB, LANES), F32),
            pltpu.VMEM((n_vert * SUB, total), F32),
            pltpu.VMEM((n_col, n_vert * SUB, comps), BF16),
            pltpu.VMEM((n_vert, 2, SUB, LANES), F32),
            pltpu.VMEM((n_vert, 2, SUB, LANES), F32),
            pltpu.VMEM((joints, SUB, LANES), F32),
            pltpu.VMEM((HALF * SUB, LANES), F32),
            pltpu.VMEM((HALF * SUB, LANES), F32),
            pltpu.VMEM((3, HALF * SUB, LANES), F32),
            pltpu.VMEM((HALF, n_vert * LANES), F32),
            dma((9,)),
            dma((n_vert,)),
            dma((n_vert,)),
            dma((n_col,)),
            dma((n_col,)),
            dma((n_vert,)),
            dma((n_vert,)),
            dma((n_vert,)),
            dma((n_vert,)),
            dma((n_vert,)),
            dma((n_vert,)),
        ],
        compiler_params=pltpu.CompilerParams(collective_id=0, has_side_effects=True),
    )(
        parents,
        coeffs,
        jnp.transpose(shape_basis, (1, 2, 0)),
        template,
        regressor,
        quaternions,
        translation,
        jnp.transpose(skin_index),
        jnp.transpose(skin_raw),
    )
    return jnp.transpose(out, (1, 0, 2)).astype(BF16)


def solution(mesh):
    in_specs = (
        P(("vert", "col"), None),
        P("col", None, "vert"),
        P(None, "vert"),
        P(None, "vert"),
        P(("vert", "col"), None, None),
        P(("vert", "col"), None),
        P(),
        P("vert", None),
        P("vert", None),
    )
    out_specs = P(("vert", "col"), None, None)
    step = functools.partial(body, mesh.shape["vert"], mesh.shape["col"])
    return jax.shard_map(step, mesh=mesh, in_specs=in_specs, out_specs=out_specs, check_vma=False)
```

```python
import functools

import jax
import jax.numpy as jnp
from jax import lax
from jax.experimental import pallas as pl
from jax.experimental.pallas import tpu as pltpu
from jax.sharding import PartitionSpec as P

MESH = pl.DeviceIdType.MESH
LANES = 128
HALF = 64
SUB = 8
F32 = jnp.float32
BF16 = jnp.bfloat16
EXACT = lax.Precision.HIGHEST


def iota(shape, dim):
    return lax.broadcasted_iota(jnp.int32, shape, dim)


def dot(a, b, precision=None):
    return jnp.dot(a, b, precision=precision, preferred_element_type=F32)


def dot_nt(a, b, precision=None):
    return lax.dot_general(a, b, (((1,), (1,)), ((), ())), precision=precision, preferred_element_type=F32)


def each(count, step):
    if count <= 16:
        for k in range(1, count):
            step(k)
    else:

        def one(k, carry):
            step(k)
            return carry

        lax.fori_loop(1, count, one, 0)


def kernel(
    n_vert,
    n_col,
    parents_hbm,
    coeffs_hbm,
    basis_hbm,
    template_hbm,
    regressor_hbm,
    quat_hbm,
    shift_hbm,
    index_hbm,
    raw_hbm,
    out_ref,
    parents,
    coeff_in,
    bas,
    template,
    regressor,
    quat,
    shift,
    index_in,
    raw_in,
    quat_rows,
    coeff_rows,
    blocks,
    sent,
    got,
    tree,
    state,
    diff,
    locals_ref,
    weights,
    local_s,
    coeff_s,
    coeff_r,
    bas_s,
    bas_r,
    index_s,
    index_r,
    raw_s,
    raw_r,
    sent_s,
    sent_r,
):
    me = lax.axis_index("vert")
    col = lax.axis_index("col")
    own, _ = coeffs_hbm.shape
    _, block, comps = basis_hbm.shape
    joints = regressor_hbm.shape[0]
    rows = n_vert * SUB

    barrier = pltpu.get_barrier_semaphore()

    def vert_peer(k):
        return (lax.rem(me + k, n_vert), col)

    def col_peer(k):
        return (me, lax.rem(col + k, n_col))

    each(n_vert, lambda k: pl.semaphore_signal(barrier, inc=1, device_id=vert_peer(k), device_id_type=MESH))
    each(n_col, lambda k: pl.semaphore_signal(barrier, inc=1, device_id=col_peer(k), device_id_type=MESH))

    pairs = [
        (coeffs_hbm, coeff_in.at[me]),
        (basis_hbm, bas.at[col]),
        (index_hbm, index_in.at[me]),
        (raw_hbm, raw_in.at[me]),
        (parents_hbm, parents),
        (quat_hbm, quat),
        (shift_hbm, shift),
        (template_hbm, template),
        (regressor_hbm, regressor),
    ]
    loads = [pltpu.make_async_copy(src, dst, local_s.at[i]) for i, (src, dst) in enumerate(pairs)]
    for load in loads:
        load.start()

    sub8 = iota((SUB, LANES), 0)
    lane8 = iota((SUB, LANES), 1)
    axis_lane = jnp.minimum((lane8 % SUB) // own, 2)
    quat_rows[...] = jnp.zeros(quat_rows.shape, F32)
    weights[...] = jnp.zeros(weights.shape, F32)
    tree[...] = jnp.zeros(tree.shape, F32)
    state[...] = jnp.zeros(state.shape, F32)
    diff[...] = jnp.zeros(diff.shape, F32)
    sent[...] = jnp.zeros(sent.shape, F32)
    for load in loads:
        load.wait()

    def copies(src, dst, send, recv, peer_of):
        def make(k):
            return pltpu.make_async_remote_copy(
                src_ref=src, dst_ref=dst, send_sem=send.at[k], recv_sem=recv.at[k], device_id=peer_of(k), device_id_type=MESH
            )

        return make

    coeff_copy = copies(coeff_in.at[me], coeff_in.at[me], coeff_s, coeff_r, vert_peer)
    bas_copy = copies(bas.at[col], bas.at[col], bas_s, bas_r, col_peer)
    index_copy = copies(index_in.at[me], index_in.at[me], index_s, index_r, vert_peer)
    raw_copy = copies(raw_in.at[me], raw_in.at[me], raw_s, raw_r, vert_peer)

    pl.semaphore_wait(barrier, n_vert + n_col - 2)
    each(n_col, lambda k: bas_copy(k).start())
    lower = 1 - me // (n_vert // 2)
    each(n_vert, lambda k: coeff_copy(k + lower * (n_vert - 2 * k)).start())
    each(n_vert, lambda k: index_copy(k).start())
    each(n_vert, lambda k: raw_copy(k).start())

    for c in range(own):
        quat_rows[4 * c : 4 * c + 4, 0:joints] = quat[c]
    q_row = iota((LANES, SUB), 0)
    q_col = iota((LANES, SUB), 1)
    w, x, y, z = [
        jnp.transpose(dot((q_col == (q_row % own) * 4 + comp).astype(F32), quat_rows[...], EXACT))[0:HALF] for comp in range(4)
    ]
    s = 2.0 / (w * w + x * x + y * y + z * z)
    matrix = [
        [1.0 - s * (y * y + z * z), s * (x * y - w * z), s * (x * z + w * y)],
        [s * (x * y + w * z), 1.0 - s * (x * x + z * z), s * (y * z - w * x)],
        [s * (x * z - w * y), s * (y * z + w * x), 1.0 - s * (x * x + y * y)],
    ]
    for m in range(3):
        for b in range(3):
            locals_ref[m, pl.ds(b, HALF, stride=SUB), :] = matrix[m][b]

    def compose(j, above):
        at = pl.multiple_of(j * SUB, SUB)
        new = jnp.zeros((SUB, LANES), F32)
        for m in range(3):
            new = new + jnp.broadcast_to(above[m : m + 1, :], (SUB, LANES)) * locals_ref[m, pl.ds(at, SUB), :]
        mine = above + (lane8 % HALF == j).astype(F32)
        new = jnp.where(sub8 < 3, new, jnp.where(sub8 == 3, mine, 0.0))
        if isinstance(j, int):
            new = new + jnp.where((sub8 == 3) & (lane8 == joints), 1.0, 0.0)
        tree[j] = new
        state[pl.ds(at, SUB), :] = new
        diff[pl.ds(at, SUB), :] = above - new

    def descend(j, carry):
        compose(j, tree[parents[j]])
        return carry

    compose(0, (axis_lane == sub8).astype(F32))
    lax.fori_loop(1, joints, descend, 0)

    def flipped(ref, m, n):
        value = ref[pl.ds(m, HALF, stride=SUB), :]
        return jnp.transpose(jnp.concatenate([value, value], axis=0))[0:n]

    gains = [flipped(diff, m, SUB) for m in range(3)]
    gains = [jnp.where(lane8 < HALF, gain, 0.0) for gain in gains]
    factors = jnp.concatenate(
        [flipped(state, m, SUB)[:, 0:HALF] for m in range(3)] + [flipped(state, 3, HALF)[:, 0:HALF]], axis=0
    )
    moves = jnp.concatenate([shift[...]] * (SUB // own), axis=0)
    m_axis = jnp.minimum(iota(moves.shape, 0) // own, 2)
    moves = jnp.sum(jnp.where(iota(moves.shape, 1) == m_axis, moves, 0.0), axis=1, keepdims=True)
    moves = jnp.where(lane8 == joints, moves, 0.0)

    each(n_vert, lambda k: coeff_copy(k).wait_recv())
    for i in range(n_vert):
        one = coeff_in[i].astype(F32)
        coeff_rows[i * SUB : (i + 1) * SUB, 0 : n_col * comps] = jnp.concatenate([one] * (SUB // own), axis=0)
    for kb in range(n_col):
        blocks[kb] = coeff_rows[:, kb * comps : (kb + 1) * comps].astype(BF16)

    totals = [template[m : m + 1, :] + dot_nt(blocks[col], bas[col, m]) for m in range(3)]
    for k in range(1, n_col):
        bas_copy(k).wait_recv()
        source = lax.rem(col + n_col - k, n_col)
        totals = [totals[m] + dot_nt(blocks[source], bas[source, m]) for m in range(3)]
    r_axis = jnp.minimum((iota((rows, block), 0) % SUB) // own, 2)
    full = jnp.where(r_axis == 0, totals[0], jnp.where(r_axis == 1, totals[1], totals[2]))
    share = dot_nt(full, regressor[...], EXACT)
    sent[:, 0, :, 0:block] = full.astype(BF16).astype(F32).reshape(n_vert, SUB, block)
    sent[:, 1, :, 0:joints] = share.reshape(n_vert, SUB, joints)

    def sent_copy(k):
        target = lax.rem(me + k, n_vert)
        return pltpu.make_async_remote_copy(
            src_ref=sent.at[target],
            dst_ref=got.at[me],
            send_sem=sent_s.at[k],
            recv_sem=sent_r.at[k],
            device_id=(target, col),
            device_id_type=MESH,
        )

    each(n_vert, lambda k: sent_copy(k + lower * (n_vert - 2 * k)).start())
    got[me] = sent[me]

    each(n_vert, lambda k: index_copy(k).wait_recv())
    each(n_vert, lambda k: raw_copy(k).wait_recv())
    joint_row = iota((HALF, block), 0)
    for i in range(n_vert):
        raw = raw_in[i]
        raw = raw / jnp.sum(raw, axis=0, keepdims=True)
        index = index_in[i]
        grid = jnp.zeros((HALF, block), F32)
        for slot in range(raw.shape[0]):
            grid = jnp.where(index[slot : slot + 1, :] == joint_row, raw[slot : slot + 1, :], grid)
        weights[:, i * LANES : i * LANES + block] = grid
    blended = dot(factors, weights[...], EXACT)
    turns = [blended[m * SUB : (m + 1) * SUB] for m in range(3)]
    upper = blended[3 * SUB :]
    upper_hi = upper.astype(BF16)
    upper_lo = (upper - upper_hi.astype(F32)).astype(BF16)
    upper_all = jnp.concatenate([upper_hi, upper_lo, upper_hi], axis=0)

    def rows_of(tile):
        spun = [tile] + [pltpu.roll(tile, own * q, 0) for q in range(1, SUB // own)]
        count = SUB // own
        result = []
        for m in range(3):
            value = spun[(-m) % count]
            for q in range(1, count):
                value = jnp.where(sub8 // own == q, spun[(q - m) % count], value)
            result.append(value)
        return result

    each(n_vert, lambda k: sent_copy(k).wait_recv())
    summed = got[0, 1]
    for i in range(1, n_vert):
        summed = summed + got[i, 1]
    places = rows_of(summed)
    term = moves
    for m in range(3):
        term = term + gains[m] * places[m]
    term_hi = term.astype(BF16)
    term_lo = (term - term_hi.astype(F32)).astype(BF16)
    term_all = jnp.concatenate([term_hi[:, 0:HALF], term_hi[:, 0:HALF], term_lo[:, 0:HALF]], axis=1)
    moved = dot(term_all, upper_all)

    n_cols = -(-n_vert * block // LANES) + 1
    columns = [None] * n_cols

    def put(q, value):
        columns[q] = value if columns[q] is None else columns[q] + value

    for i in range(n_vert):
        q, r = divmod(i * block, LANES)
        at = slice(i * LANES, (i + 1) * LANES)
        shaped = rows_of(got[i, 0])
        tile = moved[:, at]
        for m in range(3):
            tile = tile + turns[m][:, at] * shaped[m]
        if r:
            tile = pltpu.roll(tile, r, 1)
        if r + block > LANES:
            put(q, jnp.where(lane8 >= r, tile, 0.0))
            put(q + 1, jnp.where(lane8 < r, tile, 0.0))
        else:
            put(q, tile)
    width = n_vert * block
    for q in range(n_cols):
        size = min(LANES, width - q * LANES)
        if size > 0:
            value = columns[q].astype(out_ref.dtype)
            for a in range(3):
                out_ref[a, :, q * LANES : q * LANES + size] = value[own * a : own * (a + 1), 0:size]

    each(n_vert, lambda k: coeff_copy(k).wait_send())
    each(n_col, lambda k: bas_copy(k).wait_send())
    each(n_vert, lambda k: index_copy(k).wait_send())
    each(n_vert, lambda k: raw_copy(k).wait_send())
    each(n_vert, lambda k: sent_copy(k).wait_send())


def body(n_vert, n_col, coeffs, shape_basis, template, regressor, quaternions, translation, parents, skin_index, skin_raw):
    own, total = coeffs.shape
    comps, _, block = shape_basis.shape
    joints = regressor.shape[0]
    slots = skin_index.shape[1]
    vmem = pl.BlockSpec(memory_space=pltpu.VMEM)
    anywhere = pl.BlockSpec(memory_space=pl.ANY)
    dma = pltpu.SemaphoreType.DMA
    out = pl.pallas_call(
        functools.partial(kernel, n_vert, n_col),
        out_shape=jax.ShapeDtypeStruct((3, own, n_vert * block), BF16),
        in_specs=[anywhere] * 9,
        out_specs=vmem,
        scratch_shapes=[
            pltpu.SMEM((joints,), jnp.int32),
            pltpu.VMEM((n_vert, own, total), BF16),
            pltpu.VMEM((n_col, 3, block, comps), BF16),
            pltpu.VMEM((3, block), F32),
            pltpu.VMEM((joints, block), F32),
            pltpu.VMEM((own, 4, joints), F32),
            pltpu.VMEM((own, 3), F32),
            pltpu.VMEM((n_vert, slots, block), jnp.int32),
            pltpu.VMEM((n_vert, slots, block), F32),
            pltpu.VMEM((SUB, LANES), F32),
            pltpu.VMEM((n_vert * SUB, total), F32),
            pltpu.VMEM((n_col, n_vert * SUB, comps), BF16),
            pltpu.VMEM((n_vert, 2, SUB, LANES), F32),
            pltpu.VMEM((n_vert, 2, SUB, LANES), F32),
            pltpu.VMEM((joints, SUB, LANES), F32),
            pltpu.VMEM((HALF * SUB, LANES), F32),
            pltpu.VMEM((HALF * SUB, LANES), F32),
            pltpu.VMEM((3, HALF * SUB, LANES), F32),
            pltpu.VMEM((HALF, n_vert * LANES), F32),
            dma((9,)),
            dma((n_vert,)),
            dma((n_vert,)),
            dma((n_col,)),
            dma((n_col,)),
            dma((n_vert,)),
            dma((n_vert,)),
            dma((n_vert,)),
            dma((n_vert,)),
            dma((n_vert,)),
            dma((n_vert,)),
        ],
        compiler_params=pltpu.CompilerParams(collective_id=0, has_side_effects=True),
    )(
        parents,
        coeffs,
        jnp.transpose(shape_basis, (1, 2, 0)),
        template,
        regressor,
        quaternions,
        translation,
        jnp.transpose(skin_index),
        jnp.transpose(skin_raw),
    )
    return jnp.transpose(out, (1, 0, 2))


def solution(mesh):
    in_specs = (
        P(("vert", "col"), None),
        P("col", None, "vert"),
        P(None, "vert"),
        P(None, "vert"),
        P(("vert", "col"), None, None),
        P(("vert", "col"), None),
        P(),
        P("vert", None),
        P("vert", None),
    )
    out_specs = P(("vert", "col"), None, None)
    step = functools.partial(body, mesh.shape["vert"], mesh.shape["col"])
    return jax.shard_map(step, mesh=mesh, in_specs=in_specs, out_specs=out_specs, check_vma=False)
```
